32 devices in a mesh: south: 8 (over z, x), east: 4 (over y, core).
Axes of the slice: x: 2, y: 2, z: 4, core: 2. Of those that a mesh axis runs over, the one named last changes fastest.
Arguments:
- tracer: float32 [256, 128, 128], P('south', 'east'), may hold values from 0.2 to 1.8
- flow_j: float32 [256, 128, 128], P('south', 'east'), may hold values from -0.3 to 0.3
- flow_i: float32 [256, 128, 128], P('south', 'east'), may hold values from -0.3 to 0.3
Outputs:
- running_total: float32 [256, 128, 128], P('south', 'east')
- tracer_end: float32 [256, 128, 128], P('south', 'east')
The draws below stay inside these ranges and needn't reach their ends.
All inputs are finite; a program needn't handle non-finite values.
Results may differ from the reference program's by a relative error of at most 0.00002.
Values sent between devices are 32-bit elements; how exact they have to be, the bound alone decides.
A program may use at most 64 MiB of HBM per device.

```python
import jax
import jax.numpy as jnp
from jax import lax

GRID_J = 256
GRID_I = 128
MEMBERS = 128
STEPS = 4


def level_of(key, shape, pieces, least, top_value):
    gain, own = 1.0, jax.random.fold_in(key, 6)
    for dim, blocks in pieces:
        heights = jnp.exp(jax.random.uniform(jax.random.fold_in(own, dim), (blocks,), jnp.float32, least / len(pieces), top_value / len(pieces)))
        gain = gain * jnp.repeat(heights, shape[dim] // blocks).reshape([-1 if axis == dim else 1 for axis in range(len(shape))])
    return gain


def setup_inputs(seed: int = 0) -> dict:
    keys = jax.random.split(jax.random.key(seed), 4)
    tracer = jnp.clip(0.2 + 1.5999999 * jax.random.uniform(keys[0], (GRID_J, GRID_I, MEMBERS), jnp.float32) ** level_of(keys[0], (GRID_J, GRID_I, MEMBERS), ((0, 8), (1, 4)), -0.2, 0.2), 0.2, 1.8)
    flow_j = jnp.clip(jax.random.uniform(keys[1], (GRID_J, GRID_I, MEMBERS), jnp.float32, -0.3, 0.3) * level_of(keys[1], (GRID_J, GRID_I, MEMBERS), ((0, 8), (1, 4)), -0.4, 0.0), -0.3, 0.3)
    flow_i = jnp.clip(jax.random.uniform(keys[2], (GRID_J, GRID_I, MEMBERS), jnp.float32, -0.3, 0.3) * level_of(keys[2], (GRID_J, GRID_I, MEMBERS), ((0, 8), (1, 4)), -0.4, 0.0), -0.3, 0.3)
    return {"tracer": tracer, "flow_j": flow_j, "flow_i": flow_i}


def inner_cells(values, dims):
    for dim in dims:
        values = lax.slice_in_dim(values, 1, values.shape[dim] - 1, axis=dim)
    return values


def side_cells(values, dim, start, dims):
    others = [other for other in dims if other != dim]
    values = inner_cells(values, others)
    return lax.slice_in_dim(values, start, start + values.shape[dim] - 2, axis=dim)


def advance(padded, flow_j, flow_i):
    middle = inner_cells(padded, (0, 1))
    lower = [side_cells(padded, dim, 0, (0, 1)) for dim in (0, 1)]
    upper = [side_cells(padded, dim, 2, (0, 1)) for dim in (0, 1)]
    slopes = [above - below for above, below in zip(upper, lower)]
    smooth_rate = 0.05
    spread = lower[0] + upper[0] + lower[1] + upper[1] - 4.0 * middle
    return middle - flow_j * slopes[0] - flow_i * slopes[1] + smooth_rate * spread


def reference(tracer, flow_j, flow_i):
    for step in range(STEPS):
        tracer = advance(jnp.pad(tracer, ((1, 1), (1, 1), (0, 0)), mode="constant"), flow_j, flow_i)
    running_total = jnp.cumsum(tracer, axis=0) / GRID_J
    return running_total, tracer
```

```python
import functools

import jax
import jax.numpy as jnp
from jax import lax
from jax.experimental import pallas as pl
from jax.experimental.pallas import tpu as pltpu
from jax.sharding import PartitionSpec as P

STEPS = 4
TILE = 8


def chunk_of(rows, most):
    return max(c for c in range(1, most + 1) if rows % c == 0)


def advance(level, flow_j, flow_i, row, rows, col, cols):
    def at(dj, di):
        return level[pl.ds(row + 1 + dj, rows), pl.ds(col + TILE + di, cols), :]

    middle, lower_j, upper_j, lower_i, upper_i = at(0, 0), at(-1, 0), at(1, 0), at(0, -1), at(0, 1)
    fj = flow_j[pl.ds(row, rows), pl.ds(col, cols), :]
    fi = flow_i[pl.ds(row, rows), pl.ds(col, cols), :]
    spread = lower_j + upper_j + lower_i + upper_i - 4.0 * middle
    return middle - fj * (upper_j - lower_j) - fi * (upper_i - lower_i) + 0.05 * spread


def kernel(souths, easts, tracer, flow_j, flow_i, running, end, level0, level1, level2, level3, fj, fi, own, totals,
           load_sem, send_sem, recv_sem, total_send, total_recv):
    J, I, _ = tracer.shape
    s, e = lax.axis_index("south"), lax.axis_index("east")
    levels = (level0, level1, level2, level3)
    loads = [
        pltpu.make_async_copy(tracer, level0.at[pl.ds(1, J), pl.ds(TILE, I), :], load_sem.at[0]),
        pltpu.make_async_copy(flow_j, fj, load_sem.at[1]),
        pltpu.make_async_copy(flow_i, fi, load_sem.at[2]),
    ]
    for load in loads:
        load.start()

    sides = (
        (s > 0, {"south": s - 1, "east": e}),
        (s < souths - 1, {"south": s + 1, "east": e}),
        (e > 0, {"south": s, "east": e - 1}),
        (e < easts - 1, {"south": s, "east": e + 1}),
    )
    barrier = pltpu.get_barrier_semaphore()
    for exists, peer in sides[2:]:
        @pl.when(exists)
        def _(peer=peer):
            pl.semaphore_signal(barrier, inc=1, device_id=peer, device_id_type=pl.DeviceIdType.MESH)

    def greet(turn, _):
        other = lax.rem(s + turn, souths)
        pl.semaphore_signal(barrier, inc=1, device_id={"south": other, "east": e},
                            device_id_type=pl.DeviceIdType.MESH)
        return 0

    lax.fori_loop(1, souths, greet, 0)

    row_zero = jnp.zeros((1, I, tracer.shape[2]), jnp.float32)
    col_zero = jnp.zeros((J, TILE, tracer.shape[2]), jnp.float32)
    for level in levels:
        @pl.when(s == 0)
        def _(level=level):
            level[0:1, TILE:TILE + I, :] = row_zero

        @pl.when(s == souths - 1)
        def _(level=level):
            level[J + 1:J + 2, TILE:TILE + I, :] = row_zero

        @pl.when(e == 0)
        def _(level=level):
            level[1:J + 1, 0:TILE, :] = col_zero

        @pl.when(e == easts - 1)
        def _(level=level):
            level[1:J + 1, TILE + I:2 * TILE + I, :] = col_zero

    near = (e > 0).astype(jnp.int32) + (e < easts - 1).astype(jnp.int32)
    pl.semaphore_wait(barrier, souths - 1 + near)

    def copies(k):
        level = levels[k]
        own_cols, own_rows = pl.ds(TILE, I), pl.ds(1, J)
        moves = (
            ((pl.ds(1, 1), own_cols), (pl.ds(J + 1, 1), own_cols)),
            ((pl.ds(J, 1), own_cols), (pl.ds(0, 1), own_cols)),
            ((own_rows, pl.ds(TILE, TILE)), (own_rows, pl.ds(TILE + I, TILE))),
            ((own_rows, pl.ds(I, TILE)), (own_rows, pl.ds(0, TILE))),
        )
        out = []
        for side, ((exists, peer), (src, dst)) in enumerate(zip(sides, moves)):
            copy = pltpu.make_async_remote_copy(
                src_ref=level.at[src[0], src[1], :], dst_ref=level.at[dst[0], dst[1], :],
                send_sem=send_sem.at[k, side], recv_sem=recv_sem.at[k, side],
                device_id=peer, device_id_type=pl.DeviceIdType.MESH)
            out.append((exists, copy))
        return out

    def start(k, which):
        for side in which:
            exists, copy = copies(k)[side]
            pl.when(exists)(copy.start)

    def receive(k):
        for side, opposite in enumerate((1, 0, 3, 2)):
            exists = sides[side][0]
            copy = copies(k)[opposite][1]
            pl.when(exists)(copy.wait_recv)

    def put(k, row, rows, col, cols, value):
        if k == STEPS:
            end[pl.ds(row, rows), pl.ds(col, cols), :] = value
        else:
            levels[k][pl.ds(row + 1, rows), pl.ds(col + TILE, cols), :] = value

    def sweep(k, col, cols):
        rows = chunk_of(J - 2, 6)

        def body(turn, _):
            row = 1 + turn * rows
            put(k, row, rows, col, cols, advance(levels[k - 1], fj, fi, row, rows, col, cols))
            return 0

        lax.fori_loop(0, (J - 2) // rows, body, 0)

    def edge_rows(k):
        for row in (0, J - 1):
            put(k, row, 1, 0, I, advance(levels[k - 1], fj, fi, row, 1, 0, I))

    loads[0].wait()
    start(0, range(4))
    loads[1].wait()
    loads[2].wait()
    for k in range(1, STEPS + 1):
        sweep(k, TILE, I - 2 * TILE)
        receive(k - 1)
        edge_rows(k)
        if k < STEPS:
            start(k, (0, 1))
        sweep(k, 0, TILE)
        sweep(k, I - TILE, TILE)
        if k < STEPS:
            start(k, (2, 3))

    total = end[0]
    for row in range(1, J):
        total = total + end[row]
    own[...] = total

    def total_copy(source, other):
        return pltpu.make_async_remote_copy(
            src_ref=own, dst_ref=totals.at[source], send_sem=total_send.at[other], recv_sem=total_recv.at[source],
            device_id={"south": other, "east": e}, device_id_type=pl.DeviceIdType.MESH)

    def give(turn, _):
        total_copy(s, s + turn).start()
        return 0

    lax.fori_loop(1, souths - s, give, 0)

    for k in range(STEPS):
        for exists, copy in copies(k):
            pl.when(exists)(copy.wait_send)

    def take(source, state):
        total_copy(source, s).wait_recv()
        return state + totals[source]

    state = lax.fori_loop(0, s, take, jnp.zeros_like(own))
    scale = 1.0 / (J * souths)
    for row in range(J):
        state = state + end[row]
        running[row] = state * scale

    def sent(turn, _):
        total_copy(s, s + turn).wait_send()
        return 0

    lax.fori_loop(1, souths - s, sent, 0)


def per_device(souths, easts, tracer, flow_j, flow_i):
    J, I, M = tracer.shape
    out = jax.ShapeDtypeStruct((J, I, M), jnp.float32)
    return pl.pallas_call(
        functools.partial(kernel, souths, easts),
        out_shape=(out, out),
        in_specs=[pl.BlockSpec(memory_space=pl.ANY)] * 3,
        out_specs=(pl.BlockSpec(memory_space=pltpu.VMEM),) * 2,
        scratch_shapes=[pltpu.VMEM((J + 2, I + 2 * TILE, M), jnp.float32)] * STEPS
        + [pltpu.VMEM((J, I, M), jnp.float32)] * 2
        + [
            pltpu.VMEM((I, M), jnp.float32),
            pltpu.VMEM((souths, I, M), jnp.float32),
            pltpu.SemaphoreType.DMA((3,)),
            pltpu.SemaphoreType.DMA((STEPS, 4)),
            pltpu.SemaphoreType.DMA((STEPS, 4)),
            pltpu.SemaphoreType.DMA((souths,)),
            pltpu.SemaphoreType.DMA((souths,)),
        ],
        compiler_params=pltpu.CompilerParams(collective_id=0, has_side_effects=True,
                                             vmem_limit_bytes=24 * 2 ** 20),
    )(tracer, flow_j, flow_i)


def solution(mesh):
    spec = P("south", "east", None)
    body = functools.partial(per_device, mesh.shape["south"], mesh.shape["east"])
    return jax.shard_map(body, mesh=mesh, in_specs=(spec,) * 3, out_specs=(spec,) * 2, check_vma=False)
```

```python
import functools

import jax
import jax.numpy as jnp
from jax import lax
from jax.experimental import pallas as pl
from jax.experimental.pallas import tpu as pltpu
from jax.sharding import PartitionSpec as P

ROUNDS = (1, 3)
STEPS = sum(ROUNDS)
DEEP = max(ROUNDS)
TILE = 8
MESH = pl.DeviceIdType.MESH
SIDES = ((-1, 0), (1, 0), (-1, -1), (-1, 1), (1, -1), (1, 1), (0, -1), (0, 1))


def plan():
    out, base = [], 0
    for turn, depth in enumerate(ROUNDS):
        out += [(base, side, depth) for side in SIDES]
        if turn == 0:
            out += [(name, side, DEEP - 1) for name in ("fj", "fi") for side in SIDES]
        base += depth
    return [(a, side, d - 1 if all(side) else d) for a, side, d in out if d - (1 if all(side) else 0) > 0]


MESSAGES = plan()


def chunk_of(rows, most):
    return max(c for c in range(1, most + 1) if rows % c == 0)


def view(ref, row, rows, col, cols):
    return ref.at[pl.ds(row + DEEP, rows), pl.ds(col + TILE, cols), :]


def advance(level, flow_j, flow_i, *area):
    row, rows, col, cols = area

    def at(dj, di):
        return view(level, row + dj, rows, col + di, cols)[...]

    middle, lower_j, upper_j, lower_i, upper_i = at(0, 0), at(-1, 0), at(1, 0), at(0, -1), at(0, 1)
    spread = lower_j + upper_j + lower_i + upper_i - 4.0 * middle
    return (middle - view(flow_j, *area)[...] * (upper_j - lower_j)
            - view(flow_i, *area)[...] * (upper_i - lower_i) + 0.05 * spread)


def kernel(souths, easts, tracer, flow_j, flow_i, running, end, level0, level1, level2, level3, fj, fi, own, totals,
           load_sem, send_sem, recv_sem, total_send, total_recv):
    J, I, M = tracer.shape
    s, e = lax.axis_index("south"), lax.axis_index("east")
    levels = (level0, level1, level2, level3)
    arrays = {0: level0, 1: level1, 2: level2, 3: level3, "fj": fj, "fi": fi}
    loads = [pltpu.make_async_copy(src, view(dst, 0, J, 0, I), load_sem.at[k])
             for k, (src, dst) in enumerate(((tracer, level0), (flow_j, fj), (flow_i, fi)))]
    for load in loads:
        load.start()

    def exists(side):
        tests = [test for step, test in ((side[0] + 5, s > 0), (side[0] + 3, s < souths - 1),
                                         (side[1] + 5, e > 0), (side[1] + 3, e < easts - 1)) if step == 4]
        return functools.reduce(jnp.logical_and, tests)

    def peer(side):
        return {"south": s + side[0], "east": e + side[1]}

    barrier = pltpu.get_barrier_semaphore()
    near = souths - 1
    for side in SIDES:
        if side[1] and (DEEP > 1 or not side[0]):
            near = near + exists(side).astype(jnp.int32)

            @pl.when(exists(side))
            def _(side=side):
                pl.semaphore_signal(barrier, inc=1, device_id=peer(side), device_id_type=MESH)

    def greet(turn, _):
        other = lax.rem(s + turn, souths)
        pl.semaphore_signal(barrier, inc=1, device_id={"south": other, "east": e}, device_id_type=MESH)
        return 0

    lax.fori_loop(1, souths, greet, 0)

    def clear(level, depth, wide):
        for side, row, rows, col, cols in (
            ((-1, 0), -depth, depth, -wide, I + 2 * wide),
            ((1, 0), J, depth, -wide, I + 2 * wide),
            ((0, -1), -depth, J + 2 * depth, -wide, wide),
            ((0, 1), -depth, J + 2 * depth, I, wide),
        ):
            @pl.when(jnp.logical_not(exists(side)))
            def _(row=row, rows=rows, col=col, cols=cols):
                view(level, row, rows, col, cols)[...] = jnp.zeros((rows, cols, M), jnp.float32)

    base = 0
    for depth in ROUNDS:
        clear(levels[base], depth, TILE)
        base += depth
    pl.semaphore_wait(barrier, near)

    def copy_of(number):
        name, (dj, di), depth = MESSAGES[number]
        src_row, dst_row, rows = {-1: (0, J, depth), 0: (0, 0, J), 1: (J - depth, -depth, depth)}[dj]
        src_col, dst_col, cols = {-1: (0, I, TILE), 0: (0, 0, I), 1: (I - TILE, -TILE, TILE)}[di]
        return pltpu.make_async_remote_copy(
            src_ref=view(arrays[name], src_row, rows, src_col, cols),
            dst_ref=view(arrays[name], dst_row, rows, dst_col, cols),
            send_sem=send_sem.at[number], recv_sem=recv_sem.at[number],
            device_id=peer((dj, di)), device_id_type=MESH)

    def start(*names):
        for number, (name, side, _) in enumerate(MESSAGES):
            if name in names:
                pl.when(exists(side))(lambda number=number: copy_of(number).start())

    def receive(*names):
        for number, (name, side, _) in enumerate(MESSAGES):
            if name in names:
                pl.when(exists((-side[0], -side[1])))(lambda number=number: copy_of(number).wait_recv())

    def update(k, row, rows, col, cols):
        value = advance(levels[k - 1], fj, fi, row, rows, col, cols)
        if k == STEPS:
            end[pl.ds(row, rows), pl.ds(col, cols), :] = value
        else:
            view(levels[k], row, rows, col, cols)[...] = value

    def sweep(k, first, last, col, cols, most):
        rows = chunk_of(last - first, most)

        def body(turn, _):
            update(k, first + turn * rows, rows, col, cols)
            return 0

        lax.fori_loop(0, (last - first) // rows, body, 0)

    loads[0].wait()
    start(0)
    loads[1].wait()
    loads[2].wait()
    start("fj", "fi")
    base, flows_in = 0, False
    for depth in ROUNDS:
        for t in range(1, depth + 1):
            sweep(base + t, t, J - t, t, I - 2 * t, 6)
        receive(base)
        if depth > 1 and not flows_in:
            receive("fj", "fi")
            flows_in = True
        for t in range(1, depth + 1):
            m = depth - t
            sweep(base + t, -m, t, -m, I + 2 * m, 4)
            sweep(base + t, J - t, J + m, -m, I + 2 * m, 4)
            sweep(base + t, t, J - t, -m, depth, 15)
            sweep(base + t, t, J - t, I - t, depth, 15)
            if m:
                clear(levels[base + t], m, m)
        base += depth
        start(base)

    total = end[0]
    for row in range(1, J):
        total = total + end[row]
    own[...] = total

    def total_copy(source, other):
        return pltpu.make_async_remote_copy(
            src_ref=own, dst_ref=totals.at[source], send_sem=total_send.at[other], recv_sem=total_recv.at[source],
            device_id={"south": other, "east": e}, device_id_type=MESH)

    def give(turn, _):
        total_copy(s, s + turn).start()
        return 0

    lax.fori_loop(1, souths - s, give, 0)

    for number, (_, side, _) in enumerate(MESSAGES):
        pl.when(exists(side))(lambda number=number: copy_of(number).wait_send())

    def take(source, state):
        total_copy(source, s).wait_recv()
        return state + totals[source]

    state = lax.fori_loop(0, s, take, jnp.zeros_like(own))
    scale = 1.0 / (J * souths)
    for row in range(J):
        state = state + end[row]
        running[row] = state * scale

    def sent(turn, _):
        total_copy(s, s + turn).wait_send()
        return 0

    lax.fori_loop(1, souths - s, sent, 0)


def write_out(running, end, running_out, end_out, sems):
    copies = [pltpu.make_async_copy(running, running_out, sems.at[0]), pltpu.make_async_copy(end, end_out, sems.at[1])]
    for copy in copies:
        copy.start()
    for copy in copies:
        copy.wait()


def per_device(souths, easts, tracer, flow_j, flow_i):
    J, I, M = tracer.shape
    out = jax.ShapeDtypeStruct((J, I, M), jnp.float32)
    padded = pltpu.VMEM((J + 2 * DEEP, I + 2 * TILE, M), jnp.float32)
    results = pl.pallas_call(
        functools.partial(kernel, souths, easts),
        out_shape=(out, out),
        in_specs=[pl.BlockSpec(memory_space=pl.ANY)] * 3,
        out_specs=(pl.BlockSpec(memory_space=pltpu.VMEM),) * 2,
        scratch_shapes=[padded] * 6
        + [
            pltpu.VMEM((I, M), jnp.float32),
            pltpu.VMEM((souths, I, M), jnp.float32),
            pltpu.SemaphoreType.DMA((3,)),
            pltpu.SemaphoreType.DMA((len(MESSAGES),)),
            pltpu.SemaphoreType.DMA((len(MESSAGES),)),
            pltpu.SemaphoreType.DMA((souths,)),
            pltpu.SemaphoreType.DMA((souths,)),
        ],
        compiler_params=pltpu.CompilerParams(collective_id=0, has_side_effects=True,
                                             vmem_limit_bytes=105 * 2 ** 19),
    )(tracer, flow_j, flow_i)
    return pl.pallas_call(
        write_out,
        out_shape=(out, out),
        in_specs=[pl.BlockSpec(memory_space=pltpu.VMEM)] * 2,
        out_specs=(pl.BlockSpec(memory_space=pl.ANY),) * 2,
        scratch_shapes=[pltpu.SemaphoreType.DMA((2,))],
        compiler_params=pltpu.CompilerParams(vmem_limit_bytes=2 ** 20),
    )(*results)


def solution(mesh):
    spec = P("south", "east", None)
    body = functools.partial(per_device, mesh.shape["south"], mesh.shape["east"])
    return jax.shard_map(body, mesh=mesh, in_specs=(spec,) * 3, out_specs=(spec,) * 2, check_vma=False)
```

```python
import functools

import jax
import jax.numpy as jnp
from jax import lax
from jax.experimental import pallas as pl
from jax.experimental.pallas import tpu as pltpu
from jax.sharding import PartitionSpec as P

ROUNDS = (1, 3)
STEPS = sum(ROUNDS)
DEEP = max(ROUNDS)
TILE = 8
MESH = pl.DeviceIdType.MESH
SIDES = ((-1, 0), (1, 0), (-1, -1), (-1, 1), (1, -1), (1, 1), (0, -1), (0, 1))


def plan():
    out, base = [], 0
    for turn, depth in enumerate(ROUNDS):
        out += [(base, side, depth) for side in SIDES]
        if turn == 0:
            out += [(name, side, DEEP - 1) for name in ("fj", "fi") for side in SIDES]
        base += depth
    return [(a, side, d - 1 if all(side) else d) for a, side, d in out if d - (1 if all(side) else 0) > 0]


MESSAGES = plan()


def chunk_of(rows, most):
    return max(c for c in range(1, most + 1) if rows % c == 0)


def view(ref, row, rows, col, cols):
    return ref.at[pl.ds(row + DEEP, rows), pl.ds(col + TILE, cols), :]


def advance(level, flow_j, flow_i, *area):
    row, rows, col, cols = area

    def at(dj, di):
        return view(level, row + dj, rows, col + di, cols)[...]

    middle, lower_j, upper_j, lower_i, upper_i = at(0, 0), at(-1, 0), at(1, 0), at(0, -1), at(0, 1)
    spread = lower_j + upper_j + lower_i + upper_i - 4.0 * middle
    return (middle - view(flow_j, *area)[...] * (upper_j - lower_j)
            - view(flow_i, *area)[...] * (upper_i - lower_i) + 0.05 * spread)


def kernel(souths, easts, tracer, flow_j, flow_i, before, end, level0, level1, level2, level3, fj, fi, own, totals, ready,
           load_sem, send_sem, recv_sem, total_send, total_recv):
    J, I, M = tracer.shape
    s, e = lax.axis_index("south"), lax.axis_index("east")
    levels = (level0, level1, level2, level3)
    arrays = {0: level0, 1: level1, 2: level2, 3: level3, "fj": fj, "fi": fi}
    loads = [pltpu.make_async_copy(src, view(dst, 0, J, 0, I), load_sem.at[k])
             for k, (src, dst) in enumerate(((tracer, level0), (flow_j, fj), (flow_i, fi)))]
    for load in loads:
        load.start()

    def exists(side):
        tests = [test for step, test in ((side[0] + 5, s > 0), (side[0] + 3, s < souths - 1),
                                         (side[1] + 5, e > 0), (side[1] + 3, e < easts - 1)) if step == 4]
        return functools.reduce(jnp.logical_and, tests)

    def peer(side):
        return {"south": s + side[0], "east": e + side[1]}

    barrier = pltpu.get_barrier_semaphore()
    near = 0
    for side in SIDES:
        if 0 in side:
            near = near + exists(side).astype(jnp.int32)

            @pl.when(exists(side))
            def _(side=side):
                pl.semaphore_signal(barrier, inc=1, device_id=peer(side), device_id_type=MESH)

    stages = [2 ** k for k in range(1, souths.bit_length()) if 2 ** k < souths - 1]

    def tell(stage, reach):
        for ok, other in ((s >= reach, s - reach), (s + reach < souths, s + reach)):
            @pl.when(ok)
            def _(other=other):
                pl.semaphore_signal(ready.at[stage], inc=1, device_id={"south": other, "east": e}, device_id_type=MESH)

    def hear(stage, reach):
        pl.semaphore_wait(ready.at[stage], (s >= reach).astype(jnp.int32) + (s + reach < souths).astype(jnp.int32))

    def clear(level, depth, wide):
        for side, row, rows, col, cols in (
            ((-1, 0), -depth, depth, -wide, I + 2 * wide),
            ((1, 0), J, depth, -wide, I + 2 * wide),
            ((0, -1), -depth, J + 2 * depth, -wide, wide),
            ((0, 1), -depth, J + 2 * depth, I, wide),
        ):
            @pl.when(jnp.logical_not(exists(side)))
            def _(row=row, rows=rows, col=col, cols=cols):
                view(level, row, rows, col, cols)[...] = jnp.zeros((rows, cols, M), jnp.float32)

    base = 0
    for depth in ROUNDS:
        clear(levels[base], depth, TILE)
        base += depth
    pl.semaphore_wait(barrier, near)

    def copy_of(number):
        name, (dj, di), depth = MESSAGES[number]
        src_row, dst_row, rows = {-1: (0, J, depth), 0: (0, 0, J), 1: (J - depth, -depth, depth)}[dj]
        src_col, dst_col, cols = {-1: (0, I, depth), 0: (0, 0, I), 1: (I - depth, -depth, depth)}[di]
        return pltpu.make_async_remote_copy(
            src_ref=view(arrays[name], src_row, rows, src_col, cols),
            dst_ref=view(arrays[name], dst_row, rows, dst_col, cols),
            send_sem=send_sem.at[number], recv_sem=recv_sem.at[number],
            device_id=peer((dj, di)), device_id_type=MESH)

    def start(*names, corners=False):
        for number, (name, side, _) in enumerate(MESSAGES):
            if name in names and all(side) == corners:
                pl.when(exists(side))(lambda number=number: copy_of(number).start())

    def receive(*names):
        for number, (name, side, _) in enumerate(MESSAGES):
            if name in names:
                pl.when(exists((-side[0], -side[1])))(lambda number=number: copy_of(number).wait_recv())

    def update(k, row, rows, col, cols):
        value = advance(levels[k - 1], fj, fi, row, rows, col, cols)
        if k == STEPS:
            end[pl.ds(row, rows), pl.ds(col, cols), :] = value
        else:
            view(levels[k], row, rows, col, cols)[...] = value

    def sweep(k, first, last, col, cols, most):
        rows = chunk_of(last - first, most)

        def body(turn, _):
            update(k, first + turn * rows, rows, col, cols)
            return 0

        lax.fori_loop(0, (last - first) // rows, body, 0)

    loads[0].wait()
    start(0)
    loads[1].wait()
    loads[2].wait()
    start("fj", "fi")
    base = 0
    for turn, depth in enumerate(ROUNDS):
        for t in range(1, depth + 1):
            sweep(base + t, t, J - t, t, I - 2 * t, 6)
        if turn == 1 and stages:
            hear(0, stages[0])
            for stage, reach in enumerate(stages[1:], 1):
                tell(stage, reach)
                if stage < len(stages) - 1:
                    hear(stage, reach)
        receive(base)
        if turn == 0:
            start("fj", "fi", corners=True)
            if stages:
                tell(0, stages[0])
        if turn == 1:
            receive("fj", "fi")
        for t in range(1, depth + 1):
            m = depth - t
            sweep(base + t, -m, t, -m, I + 2 * m, 4)
            sweep(base + t, J - t, J + m, -m, I + 2 * m, 4)
            sweep(base + t, t, J - t, -m, depth, 15)
            sweep(base + t, t, J - t, I - t, depth, 15)
            if m:
                clear(levels[base + t], m, m)
        base += depth
        start(base)
        start(base, corners=True)
    if len(stages) > 1:
        hear(len(stages) - 1, stages[-1])

    total = end[0]
    for row in range(1, J):
        total = total + end[row]
    own[...] = total

    def total_copy(source, other):
        return pltpu.make_async_remote_copy(
            src_ref=own, dst_ref=totals.at[source], send_sem=total_send.at[other], recv_sem=total_recv.at[source],
            device_id={"south": other, "east": e}, device_id_type=MESH)

    def give(turn, _):
        total_copy(s, s + turn).start()
        return 0

    lax.fori_loop(1, souths - s, give, 0)

    for number, (_, side, _) in enumerate(MESSAGES):
        pl.when(exists(side))(lambda number=number: copy_of(number).wait_send())

    def take(source, state):
        total_copy(source, s).wait_recv()
        return state + totals[source]

    before[...] = lax.fori_loop(0, s, take, jnp.zeros_like(own))

    def sent(turn, _):
        total_copy(s, s + turn).wait_send()
        return 0

    lax.fori_loop(1, souths - s, sent, 0)


def write_out(scale, before, end, running_out, end_out, running, sems):
    J = end.shape[0]
    rows = chunk_of(J, 8)
    copies = [pltpu.make_async_copy(end, end_out, sems.at[0])]
    copies[0].start()
    state = before[...]
    for chunk in range(J // rows):
        for row in range(chunk * rows, (chunk + 1) * rows):
            state = state + end[row]
            running[row] = state * scale
        part = pl.ds(chunk * rows, rows)
        copies.append(pltpu.make_async_copy(running.at[part], running_out.at[part], sems.at[1 + chunk]))
        copies[-1].start()
    for copy in copies:
        copy.wait()


def per_device(souths, easts, tracer, flow_j, flow_i):
    J, I, M = tracer.shape
    out = jax.ShapeDtypeStruct((J, I, M), jnp.float32)
    padded = pltpu.VMEM((J + 2 * DEEP, I + 2 * TILE, M), jnp.float32)
    results = pl.pallas_call(
        functools.partial(kernel, souths, easts),
        out_shape=(jax.ShapeDtypeStruct((I, M), jnp.float32), out),
        in_specs=[pl.BlockSpec(memory_space=pl.ANY)] * 3,
        out_specs=(pl.BlockSpec(memory_space=pltpu.VMEM),) * 2,
        scratch_shapes=[padded] * 6
        + [
            pltpu.VMEM((I, M), jnp.float32),
            pltpu.VMEM((souths, I, M), jnp.float32),
            pltpu.SemaphoreType.REGULAR((souths.bit_length(),)),
            pltpu.SemaphoreType.DMA((3,)),
            pltpu.SemaphoreType.DMA((len(MESSAGES),)),
            pltpu.SemaphoreType.DMA((len(MESSAGES),)),
            pltpu.SemaphoreType.DMA((souths,)),
            pltpu.SemaphoreType.DMA((souths,)),
        ],
        compiler_params=pltpu.CompilerParams(collective_id=0, has_side_effects=True,
                                             vmem_limit_bytes=106 * 2 ** 19),
    )(tracer, flow_j, flow_i)
    return pl.pallas_call(
        functools.partial(write_out, 1.0 / (J * souths)),
        out_shape=(out, out),
        in_specs=[pl.BlockSpec(memory_space=pltpu.VMEM)] * 2,
        out_specs=(pl.BlockSpec(memory_space=pl.ANY),) * 2,
        scratch_shapes=[pltpu.VMEM((J, I, M), jnp.float32), pltpu.SemaphoreType.DMA((J + 1,))],
        compiler_params=pltpu.CompilerParams(vmem_limit_bytes=2 ** 21),
    )(*results)


def solution(mesh):
    spec = P("south", "east", None)
    body = functools.partial(per_device, mesh.shape["south"], mesh.shape["east"])
    return jax.shard_map(body, mesh=mesh, in_specs=(spec,) * 3, out_specs=(spec,) * 2, check_vma=False)
```
